32 devices in a mesh: dp: 8 (over z, x), tensor: 4 (over y, core).
Axes of the slice: x: 2, y: 2, z: 4, core: 2. Of those that a mesh axis runs over, the one named last changes fastest.
Arguments:
- tokens: bfloat16 [20480, 768], P(('dp', 'tensor')), may hold values from -6 to 6
- cotangent: bfloat16 [20480, 768], P(('dp', 'tensor')), may hold values from -6 to 6
- lengths: int32 [8, 8], P('dp'), may hold values from 1 to 512, 2048 in all within a row
- w_qkv: bfloat16 [768, 3, 768], P('dp', None, 'tensor'), may hold values from -0.21875 to 0.21875
- w_out: bfloat16 [768, 768], P('tensor', 'dp'), may hold values from -6 to 6
- w_fc: bfloat16 [768, 3072], P('dp', 'tensor'), may hold values from -0.21875 to 0.21875
- w_proj: bfloat16 [3072, 768], P('tensor', 'dp'), may hold values from -0.109375 to 0.109375
- ln1_gain: bfloat16 [768], P('dp'), may hold values from 0.25 to 1.75
- ln1_bias: bfloat16 [768], P('dp'), may hold values from -3 to 3
- ln2_gain: bfloat16 [768], P('dp'), may hold values from 0.25 to 1.75
- ln2_bias: bfloat16 [768], P('dp'), may hold values from -3 to 3
Outputs:
- block_out: bfloat16 [20480, 768], P(('dp', 'tensor'))
- input_grad: bfloat16 [20480, 768], P(('dp', 'tensor'))
- w_qkv_grad: float32 [768, 3, 768], P('dp', None, 'tensor')
- w_out_grad: float32 [768, 768], P('tensor', 'dp')
- w_fc_grad: float32 [768, 3072], P('dp', 'tensor')
- w_proj_grad: float32 [3072, 768], P('tensor', 'dp')
- ln1_gain_grad: float32 [768], P('dp')
- ln1_bias_grad: float32 [768], P('dp')
- ln2_gain_grad: float32 [768], P('dp')
- ln2_bias_grad: float32 [768], P('dp')
The draws below stay inside these ranges and needn't reach their ends.
Inputs may be any that keep to these rules, and one draw needn't show every extreme that they name: `lengths`: row g lists the token counts of group g's 8 continuations in order after its 512-token prompt; each row sums to 2048 and its largest entry is exactly 512.
All inputs are finite; a program needn't handle non-finite values.
Results may differ from the reference program's by a relative error of at most 0.019.
The reference program's roundings to bfloat16 on the way count: a program that leaves them out, or rounds other values in their place, can miss the bound.
Values may be sent and summed in bfloat16 or wider, within the bound.
A program may use at most 192 MiB of HBM per device.

```python
import math
import jax
import jax.numpy as jnp
import numpy as np
from jax import lax

D = 768
HEADS = 12
HEAD = 64
FF = 3072
PROMPT = 512
NCONT = 8
CONT_TOK = 2048
CONT_MOST = 512
GROUP = 2560
GROUPS = 8
TOKENS = 20480


def with_spikes(array, own_key, source, target, shards_of, factor):
    def block_of(dim):
        return (jnp.arange(array.shape[dim]) // (array.shape[dim] // shards_of)).reshape((-1,) + (1,) * (array.ndim - 1 - dim))

    near = jax.random.permutation(own_key, shards_of)[block_of(target)]
    second = (block_of(target) + shards_of // 2) % shards_of
    return jnp.where((block_of(source) == near) | (block_of(source) == second), factor * array, array)


def steps_of(own_key, shape, pieces, low, high):
    def one(position, shards_of):
        heights = jax.random.uniform(jax.random.fold_in(jax.random.fold_in(own_key, 6), position), (shards_of,), jnp.float32, low / len(pieces), high / len(pieces))
        return jnp.repeat(jnp.exp(heights), shape[position] // shards_of).reshape((-1,) + (1,) * (len(shape) - position - 1))

    factor_of = one(*pieces[0])
    for cut in pieces[1:]:
        factor_of = factor_of * one(*cut)
    return factor_of


def length_profile(amount, total, limit, skew):
    loads = [(1 << 20) // math.isqrt(standing ** skew) + 1 for standing in range(2, amount + 1)]
    rest, given = total - limit - (amount - 1), [1] * (amount - 1)
    while rest > 0:
        candidates = [i for i in range(amount - 1) if given[i] < limit]
        whole, remaining = sum([loads[i] for i in candidates]), rest
        for i in candidates:
            more = min(limit - given[i], max(1, remaining * loads[i] // whole), rest)
            given[i] = given[i] + more
            rest = rest - more
    return np.array([limit] + given)


def ragged(stream_key, amount, total, reach, skew):
    if amount == 2:
        one = jax.random.randint(stream_key, (), max(1, total - reach), min(reach, total - 1) + 1)
        return jnp.stack([one, total - one])
    sizes = jnp.asarray(length_profile(amount, total, reach, skew), jnp.int32)
    pairs = (amount - 1) // 2
    donor, receiver = sizes[1:1 + 2 * pairs:2], sizes[2:2 + 2 * pairs:2]
    margin = jnp.minimum(donor - 1, reach - receiver)
    moved = jax.random.randint(jax.random.fold_in(stream_key, 1), (pairs,), 0, 1 << 20) % (margin + 1)
    sizes = sizes.at[1:1 + 2 * pairs:2].set(donor - moved).at[2:2 + 2 * pairs:2].set(receiver + moved)
    return sizes[jax.random.permutation(jax.random.fold_in(stream_key, 2), amount)]


def gaussian(rng, shape, scale, limit, split=(), kind=jnp.bfloat16):
    array = scale * jax.random.normal(rng, shape, jnp.float32)
    if split:
        array = array * steps_of(rng, shape, split, -0.22, 0.18)
    return jnp.clip(array, -limit, limit).astype(kind)


def noise_with(own_key, extent, deviation, bound, split, heavy, kind=jnp.bfloat16):
    array = deviation * jax.random.normal(own_key, extent, jnp.float32)
    if split:
        array = array * steps_of(own_key, extent, split, -0.22, 0.18)
    return jnp.clip(with_spikes(array, jax.random.fold_in(own_key, 3), *heavy), -bound, bound).astype(kind)


def setup_inputs(seed: int = 0) -> dict:
    streams_of = jax.random.split(jax.random.key(seed), 12)
    return {
        "tokens": gaussian(streams_of[0], (TOKENS, D), 1.0, 6.0, ((0, 32),)),
        "cotangent": noise_with(streams_of[1], (TOKENS, D), 1.0, 6.0, ((0, 32),), (0, 1, 32, 2.75)),
        "lengths": jax.vmap(lambda own: ragged(own, NCONT, CONT_TOK, CONT_MOST, 2))(jax.random.split(streams_of[2], GROUPS)).reshape((GROUPS, NCONT)).astype(jnp.int32),
        "w_qkv": gaussian(streams_of[3], (D, 3, D), D ** -0.5, 0.21875, ((0, 8), (2, 4))),
        "w_out": gaussian(streams_of[4], (D, D), 1.0, 6.0, ((0, 4), (1, 8))),
        "w_fc": gaussian(streams_of[5], (D, FF), D ** -0.5, 0.21875, ((0, 8), (1, 4))),
        "w_proj": gaussian(streams_of[6], (FF, D), FF ** -0.5, 0.109375, ((0, 4), (1, 8))),
        "ln1_gain": jnp.clip(1.0 + 0.15 * jax.random.normal(streams_of[7], (D,), jnp.float32), 0.25, 1.75).astype(jnp.bfloat16),
        "ln1_bias": gaussian(streams_of[8], (D,), 0.3, 3.0, ((0, 8),)),
        "ln2_gain": jnp.clip(1.0 + 0.15 * jax.random.normal(streams_of[9], (D,), jnp.float32), 0.25, 1.75).astype(jnp.bfloat16),
        "ln2_bias": gaussian(streams_of[10], (D,), 0.3, 3.0, ((0, 8),)),
    }


@jax.custom_vjp
def low(v):
    return lax.optimization_barrier(v.astype(jnp.bfloat16)).astype(jnp.float32)

@jax.custom_vjp
def low_back(v):
    return v

def low_keep(v):
    return (low(v), None)

def low_pass(kept, grad):
    return (grad,)

def back_keep(v):
    return (v, None)

def back_low(kept, grad):
    return (low(grad),)
low.defvjp(low_keep, low_pass)
low_back.defvjp(back_keep, back_low)

def layer_norm(values, gain, bias):
    mean = lax.optimization_barrier(jnp.mean(values, axis=-1, keepdims=True))
    centred = values - mean
    spread = lax.optimization_barrier(jnp.mean(centred * centred, axis=-1, keepdims=True))
    return centred * lax.rsqrt(spread + 1e-05) * gain + bias

def matmul(left, right):
    return jnp.dot(left, right, precision=lax.Precision.HIGHEST, preferred_element_type=jnp.float32)

def attention(queries, keys, values, places, segs):
    total = queries.shape[0]
    block = total // max(1, total // 512)
    count = total // block
    scale = HEAD ** (-0.5)

    def one(index):
        start = index * block
        query = lax.dynamic_slice_in_dim(queries, start, block, 0)
        query_pos = lax.dynamic_slice_in_dim(places, start, block, 0)
        query_seg = lax.dynamic_slice_in_dim(segs, start, block, 0)
        causal = places[None, :] <= query_pos[:, None]
        shared = (segs[None, :] < 0) | (segs[None, :] == query_seg[:, None])
        mask = (causal & shared)[None]
        raw = low_back(jnp.einsum('qhd,khd->hqk', query, keys, precision=lax.Precision.HIGHEST) * scale)
        magnitude = jnp.where(mask, jnp.abs(raw), -1e+30)
        top = lax.optimization_barrier(jnp.max(magnitude, axis=-1, keepdims=True))
        expo = jnp.where(mask, jnp.exp(magnitude - top), 0.0)
        prob = expo / lax.optimization_barrier(jnp.sum(expo, axis=-1, keepdims=True))
        weights = low(jnp.sign(raw) * prob)
        return jnp.einsum('hqk,khd->qhd', weights, values, precision=lax.Precision.HIGHEST)
    mixed = lax.map(jax.checkpoint(one), jnp.arange(count, dtype=jnp.int32))
    return mixed.reshape(total, HEADS * HEAD)

def group_forward(inputs, places, segs, params):
    w_qkv, w_out, w_fc, w_proj, gain1, bias1, gain2, bias2 = params
    total = inputs.shape[0]
    lowered1 = low(layer_norm(inputs, gain1, bias1))
    projected = low_back(low(matmul(lowered1, w_qkv.reshape(D, 3 * D)))).reshape(total, 3, HEADS, HEAD)
    mixed = attention(projected[:, 0], projected[:, 1], projected[:, 2], places, segs)
    mixed = low_back(low(mixed))
    resid = inputs + low_back(matmul(mixed, w_out))
    lowered2 = low(layer_norm(resid, gain2, bias2))
    hidden = low(jax.nn.gelu(low_back(matmul(lowered2, w_fc)), approximate=True))
    return resid + matmul(hidden, w_proj)

def reference(tokens, cotangent, lengths, w_qkv, w_out, w_fc, w_proj, ln1_gain, ln1_bias, ln2_gain, ln2_bias):
    params = (w_qkv.astype(jnp.float32), w_out.astype(jnp.float32), w_fc.astype(jnp.float32), w_proj.astype(jnp.float32), ln1_gain.astype(jnp.float32), ln1_bias.astype(jnp.float32), ln2_gain.astype(jnp.float32), ln2_bias.astype(jnp.float32))
    inputs = tokens.astype(jnp.float32).reshape(GROUPS, GROUP, D)
    grads_out = cotangent.astype(jnp.float32).reshape(GROUPS, GROUP, D)
    ends = (PROMPT + jnp.cumsum(lengths, axis=1)).astype(jnp.int32)
    places = jnp.arange(GROUP, dtype=jnp.int32)
    passed = lax.optimization_barrier(jnp.sum((places[None, :, None] >= ends[:, None, :]).astype(jnp.int32), axis=2))
    segs = jnp.where(places[None, :] < PROMPT, -1, passed).astype(jnp.int32)

    def forward(values, weights):

        def one(pair):
            return jax.checkpoint(group_forward)(pair[0], places, pair[1], weights)
        return lax.map(one, (values, segs))
    outputs, pull = jax.vjp(forward, inputs, params)
    input_grad, grads = pull(grads_out)
    qkv_grad, out_grad, fc_grad, proj_grad, gain1_grad, bias1_grad, gain2_grad, bias2_grad = grads
    return (outputs.reshape(TOKENS, D).astype(jnp.bfloat16), input_grad.reshape(TOKENS, D).astype(jnp.bfloat16), qkv_grad, out_grad, fc_grad, proj_grad, gain1_grad, bias1_grad, gain2_grad, bias2_grad)
```

```python
import functools

import jax
import jax.numpy as jnp
from jax import lax
from jax.experimental import pallas as pl
from jax.experimental.pallas import tpu as pltpu
from jax.sharding import PartitionSpec as P

HEAD = 64
PROMPT = 512
TILE = 256
REACH = 2
BIG = 3.0e38


def nt(left, right):
    return lax.dot_general(left, right, (((1,), (1,)), ((), ())), preferred_element_type=jnp.float32)


def nn(left, right):
    return jnp.dot(left, right, preferred_element_type=jnp.float32)


def first_of(lengths_ref, total):
    places = lax.broadcasted_iota(jnp.int32, (1, total), 1)
    first = jnp.zeros((1, total), jnp.int32)
    begin = jnp.int32(PROMPT)
    for c in range(lengths_ref.shape[1]):
        first = jnp.where(places >= begin, begin, first)
        begin = begin + lengths_ref[0, c]
    return first


def key_parts(index):
    if isinstance(index, int) and index < PROMPT // TILE:
        return [(j * TILE, j == index, False) for j in range(index + 1)]
    parts = [(j * TILE, False, False) for j in range(PROMPT // TILE)]
    if isinstance(index, int):
        band = range(max(PROMPT // TILE, index - REACH), index + 1)
        return parts + [(j * TILE, j == index, True) for j in band]
    return parts + [((index - r) * TILE, r == 0, True) for r in range(REACH, -1, -1)]


def seen(key0, query0, first, diagonal, banded):
    keys = key0 + lax.broadcasted_iota(jnp.int32, (TILE, TILE), 0)
    mask = None
    if banded:
        mask = keys >= first
    if diagonal:
        causal = keys <= query0 + lax.broadcasted_iota(jnp.int32, (TILE, TILE), 1)
        mask = causal if mask is None else mask & causal
    return mask


def rows(ref, start):
    return ref[pl.ds(start if isinstance(start, int) else pl.multiple_of(start, TILE), TILE), :]


def cols(ref, start):
    return ref[:, pl.ds(start if isinstance(start, int) else pl.multiple_of(start, TILE), TILE)]


def signs(values):
    return jnp.clip(values * BIG, -1.0, 1.0)


def each_tile(count, body):
    steady = PROMPT // TILE + REACH
    for index in range(min(steady, count)):
        body(index)
    if count > steady:
        lax.fori_loop(steady, count, lambda i, c: (body(i), c)[1], 0)


def forward_kernel(heads, lengths_ref, qkv_ref, mixed_ref, lse_ref, q_s, k_s, vt_s, o_s, first_s):
    total = qkv_ref.shape[0]
    local = heads * HEAD
    head = pl.program_id(0)

    @pl.when(head == 0)
    def _():
        first_s[...] = first_of(lengths_ref, total)

    for h in range(heads):
        @pl.when(head == h)
        def _(h=h):
            at = h * HEAD
            q_s[...] = qkv_ref[:, at : at + HEAD] * jnp.bfloat16(HEAD**-0.5)
            k_s[...] = qkv_ref[:, local + at : local + at + HEAD]
            vt_s[...] = qkv_ref[:, 2 * local + at : 2 * local + at + HEAD].T

    def body(index):
        query0 = index * TILE
        query = rows(q_s, query0)
        first = cols(first_s, query0)
        raws, sizes, tops = [], [], []
        parts = key_parts(index)
        for key0, diagonal, banded in parts:
            raw = nt(rows(k_s, key0), query)
            size = jnp.abs(raw)
            mask = seen(key0, query0, first, diagonal, banded)
            if mask is not None:
                size = jnp.where(mask, size, -1e30)
            raws.append(raw)
            sizes.append(size)
            tops.append(jnp.max(size, axis=0, keepdims=True))
        top = functools.reduce(jnp.maximum, tops)
        expos = [jnp.exp(size - top) for size in sizes]
        total_e = functools.reduce(jnp.add, [jnp.sum(e, axis=0, keepdims=True) for e in expos])
        inverse = 1.0 / total_e
        acc = None
        for (key0, _, _), raw, expo in zip(parts, raws, expos):
            weight = (signs(raw) * (expo * inverse)).astype(jnp.bfloat16)
            term = nn(cols(vt_s, key0), weight)
            acc = term if acc is None else acc + term
        o_s[pl.ds(query0, TILE), :] = acc.T.astype(jnp.bfloat16)
        lse_ref[0, :, pl.ds(query0, TILE)] = top + jnp.log(total_e)

    each_tile(total // TILE, body)
    for h in range(heads):
        @pl.when(head == h)
        def _(h=h):
            mixed_ref[:, h * HEAD : (h + 1) * HEAD] = o_s[...]


def whole(shape):
    return pl.BlockSpec(shape, lambda *_: (0,) * len(shape), pipeline_mode=pl.Buffered(1))


def attend(qkv, lengths, heads):
    total = qkv.shape[0]
    return pl.pallas_call(
        functools.partial(forward_kernel, heads),
        grid=(heads,),
        in_specs=[pl.BlockSpec(memory_space=pltpu.SMEM), whole(qkv.shape)],
        out_specs=[whole((total, heads * HEAD)), pl.BlockSpec((1, 1, total), lambda h: (h, 0, 0))],
        out_shape=[
            jax.ShapeDtypeStruct((total, heads * HEAD), jnp.bfloat16),
            jax.ShapeDtypeStruct((heads, 1, total), jnp.float32),
        ],
        scratch_shapes=[
            pltpu.VMEM((total, HEAD), jnp.bfloat16),
            pltpu.VMEM((total, HEAD), jnp.bfloat16),
            pltpu.VMEM((HEAD, total), jnp.bfloat16),
            pltpu.VMEM((total, HEAD), jnp.bfloat16),
            pltpu.VMEM((1, total), jnp.int32),
        ],
        compiler_params=pltpu.CompilerParams(vmem_limit_bytes=48 << 20),
        name="attend",
    )(lengths, qkv)


def backward_kernel(
    heads, lengths_ref, qkv_ref, mixed_ref, dmix_ref, lse_ref, grad_ref,
    q_s, k_s, kt_s, v_s, d_s, delta_s, dq_s, dk_s, dv_s, first_s,
):
    total = qkv_ref.shape[0]
    local = heads * HEAD
    head = pl.program_id(0)
    scale = HEAD**-0.5

    @pl.when(head == 0)
    def _():
        first_s[...] = first_of(lengths_ref, total)

    for h in range(heads):
        @pl.when(head == h)
        def _(h=h):
            at = h * HEAD
            q_s[...] = qkv_ref[:, at : at + HEAD] * jnp.bfloat16(scale)
            key = qkv_ref[:, local + at : local + at + HEAD]
            k_s[...] = key
            kt_s[...] = key.T
            v_s[...] = qkv_ref[:, 2 * local + at : 2 * local + at + HEAD]
            grad = dmix_ref[:, at : at + HEAD]
            d_s[...] = grad
            product = grad.astype(jnp.float32) * mixed_ref[:, at : at + HEAD].astype(jnp.float32)
            delta_s[...] = jnp.sum(product.T, axis=0, keepdims=True)

    dk_s[...] = jnp.zeros_like(dk_s)
    dv_s[...] = jnp.zeros_like(dv_s)

    def body(index):
        query0 = index * TILE
        query = rows(q_s, query0)
        grad = rows(d_s, query0)
        first = cols(first_s, query0)
        lse = lse_ref[0, :, pl.ds(query0, TILE)]
        inner = cols(delta_s, query0)
        acc = None
        for key0, diagonal, banded in key_parts(index):
            raw = nt(rows(k_s, key0), query)
            prob = jnp.exp(jnp.abs(raw) - lse)
            mask = seen(key0, query0, first, diagonal, banded)
            if mask is not None:
                prob = jnp.where(mask, prob, 0.0)
            signed = signs(raw) * prob
            wgrad = nt(rows(v_s, key0), grad)
            sgrad = (prob * wgrad - signed * inner).astype(jnp.bfloat16)
            at = pl.ds(key0, TILE)
            dv_s[at, :] = dv_s[at, :] + nn(signed.astype(jnp.bfloat16), grad)
            dk_s[at, :] = dk_s[at, :] + nn(sgrad, query)
            term = nn(cols(kt_s, key0), sgrad)
            acc = term if acc is None else acc + term
        dq_s[pl.ds(query0, TILE), :] = (acc * scale).T.astype(jnp.bfloat16)

    each_tile(total // TILE, body)
    for h in range(heads):
        @pl.when(head == h)
        def _(h=h):
            at = h * HEAD
            grad_ref[:, at : at + HEAD] = dq_s[...]
            grad_ref[:, local + at : local + at + HEAD] = dk_s[...].astype(jnp.bfloat16)
            grad_ref[:, 2 * local + at : 2 * local + at + HEAD] = dv_s[...].astype(jnp.bfloat16)


def attend_back(qkv, mixed, dmix, lse, lengths, heads):
    total = qkv.shape[0]
    low = jnp.bfloat16
    return pl.pallas_call(
        functools.partial(backward_kernel, heads),
        grid=(heads,),
        in_specs=[
            pl.BlockSpec(memory_space=pltpu.SMEM), whole(qkv.shape), whole(mixed.shape), whole(dmix.shape),
            pl.BlockSpec((1, 1, total), lambda h: (h, 0, 0)),
        ],
        out_specs=whole(qkv.shape),
        out_shape=jax.ShapeDtypeStruct(qkv.shape, low),
        scratch_shapes=[
            pltpu.VMEM((total, HEAD), low), pltpu.VMEM((total, HEAD), low), pltpu.VMEM((HEAD, total), low),
            pltpu.VMEM((total, HEAD), low), pltpu.VMEM((total, HEAD), low), pltpu.VMEM((1, total), jnp.float32),
            pltpu.VMEM((total, HEAD), low), pltpu.VMEM((total, HEAD), jnp.float32),
            pltpu.VMEM((total, HEAD), jnp.float32), pltpu.VMEM((1, total), jnp.int32),
        ],
        compiler_params=pltpu.CompilerParams(vmem_limit_bytes=48 << 20),
        name="attend_back",
    )(lengths, qkv, mixed, dmix, lse)


def normalize(values):
    mean = jnp.mean(values, axis=-1, keepdims=True)
    centred = values - mean
    spread = jnp.mean(centred * centred, axis=-1, keepdims=True)
    factor = lax.rsqrt(spread + 1e-05)
    return (centred * factor, factor)


def norm_back(grad_out, normed, factor, gain):
    scaled = grad_out * gain
    first = jnp.mean(scaled, axis=-1, keepdims=True)
    second = jnp.mean(scaled * normed, axis=-1, keepdims=True)
    return factor * (scaled - first - normed * second)


def gelu_tanh(values):
    return jax.nn.gelu(values, approximate=True)


def inner_rows(left, right):
    return lax.dot_general(
        left, right, (((0,), (0,)), ((), ())), preferred_element_type=jnp.float32
    )


def times_trans(left, right):
    return lax.dot_general(
        left, right, (((1,), (1,)), ((), ())), preferred_element_type=jnp.float32
    )


def on_device(
    tokens, cotangent, lengths, w_qkv, w_out, w_fc, w_proj, ln1_gain, ln1_bias, ln2_gain, ln2_bias
):
    rows = tokens.shape[0]
    group = rows * lax.axis_size("tensor")
    pieces = (w_qkv, w_out, w_fc, w_proj, ln1_gain, ln1_bias, ln2_gain, ln2_bias)
    qkv_full, out_full, fc_full, proj_full, gain1, bias1, gain2, bias2 = (
        lax.all_gather(pieces[0], "dp", axis=0, tiled=True),
        lax.all_gather(pieces[1], "dp", axis=1, tiled=True),
        lax.all_gather(pieces[2], "dp", axis=0, tiled=True),
        lax.all_gather(pieces[3], "dp", axis=1, tiled=True),
        lax.all_gather(pieces[4], "dp", axis=0, tiled=True),
        lax.all_gather(pieces[5], "dp", axis=0, tiled=True),
        lax.all_gather(pieces[6], "dp", axis=0, tiled=True),
        lax.all_gather(pieces[7], "dp", axis=0, tiled=True),
    )
    gain1 = gain1.astype(jnp.float32)
    bias1 = bias1.astype(jnp.float32)
    gain2 = gain2.astype(jnp.float32)
    bias2 = bias2.astype(jnp.float32)
    width = qkv_full.shape[0]
    local = qkv_full.shape[2]
    heads = local // HEAD
    qkv_mat = qkv_full.reshape(width, 3 * local)
    inputs = tokens.astype(jnp.float32)
    normed1, factor1 = normalize(inputs)
    lowered1 = (normed1 * gain1 + bias1).astype(jnp.bfloat16)
    all_norm1 = lax.all_gather(lowered1, "tensor", axis=0, tiled=True)
    projected = jnp.dot(all_norm1, qkv_mat, preferred_element_type=jnp.float32).astype(jnp.bfloat16)
    mixed, sums = attend(projected, lengths, heads)
    part = mixed
    resid = inputs + lax.psum_scatter(
        jnp.dot(part, out_full, preferred_element_type=jnp.float32).astype(jnp.bfloat16),
        "tensor",
        scatter_dimension=0,
        tiled=True,
    ).astype(jnp.float32)
    normed2, factor2 = normalize(resid)
    lowered2 = (normed2 * gain2 + bias2).astype(jnp.bfloat16)
    all_norm2 = lax.all_gather(lowered2, "tensor", axis=0, tiled=True)
    hidden_pre = jnp.dot(all_norm2, fc_full, preferred_element_type=jnp.float32)
    hidden, gelu_pull = jax.vjp(gelu_tanh, hidden_pre)
    hidden_low = hidden.astype(jnp.bfloat16)
    part = hidden_low
    mlp_rows = lax.psum_scatter(
        jnp.dot(part, proj_full, preferred_element_type=jnp.float32).astype(jnp.bfloat16),
        "tensor",
        scatter_dimension=0,
        tiled=True,
    ).astype(jnp.float32)
    block_out = (resid + mlp_rows).astype(jnp.bfloat16)
    grad_all = lax.all_gather(cotangent, "tensor", axis=0, tiled=True)
    hidden_grad = times_trans(grad_all, proj_full)
    proj_grad = inner_rows(hidden_low, grad_all)
    pre_low = gelu_pull(hidden_grad)[0].astype(jnp.bfloat16)
    fc_grad = inner_rows(all_norm2, pre_low)
    part = pre_low
    norm2_grad = lax.psum_scatter(
        times_trans(part, fc_full).astype(jnp.bfloat16), "tensor", scatter_dimension=0, tiled=True
    ).astype(jnp.float32)
    gain2_part = jnp.sum(norm2_grad * normed2, axis=0)
    bias2_part = jnp.sum(norm2_grad, axis=0)
    resid_grad = cotangent.astype(jnp.float32) + norm_back(norm2_grad, normed2, factor2, gain2)
    resid_low = resid_grad.astype(jnp.bfloat16)
    resid_all = lax.all_gather(resid_low, "tensor", axis=0, tiled=True)
    out_grad = inner_rows(mixed, resid_all)
    mixed_grad = times_trans(resid_all, out_full).astype(jnp.bfloat16)
    qkv_grad_low = attend_back(projected, mixed, mixed_grad, sums, lengths, heads)
    qkv_grad = inner_rows(all_norm1, qkv_grad_low).reshape(width, 3, local)
    part = qkv_grad_low
    norm1_grad = lax.psum_scatter(
        times_trans(part, qkv_mat).astype(jnp.bfloat16), "tensor", scatter_dimension=0, tiled=True
    ).astype(jnp.float32)
    gain1_part = jnp.sum(norm1_grad * normed1, axis=0)
    bias1_part = jnp.sum(norm1_grad, axis=0)
    input_grad = (resid_grad + norm_back(norm1_grad, normed1, factor1, gain1)).astype(jnp.bfloat16)
    qkv_sum, out_sum, fc_sum, proj_sum, gain1_share, bias1_share, gain2_share, bias2_share = (
        lax.psum_scatter(qkv_grad, "dp", scatter_dimension=0, tiled=True),
        lax.psum_scatter(out_grad, "dp", scatter_dimension=1, tiled=True),
        lax.psum_scatter(fc_grad, "dp", scatter_dimension=0, tiled=True),
        lax.psum_scatter(proj_grad, "dp", scatter_dimension=1, tiled=True),
        lax.psum_scatter(gain1_part, "dp", scatter_dimension=0, tiled=True),
        lax.psum_scatter(bias1_part, "dp", scatter_dimension=0, tiled=True),
        lax.psum_scatter(gain2_part, "dp", scatter_dimension=0, tiled=True),
        lax.psum_scatter(bias2_part, "dp", scatter_dimension=0, tiled=True),
    )
    gain1_sum, bias1_sum, gain2_sum, bias2_sum = lax.psum(
        (gain1_share, bias1_share, gain2_share, bias2_share), "tensor"
    )
    return (
        block_out,
        input_grad,
        qkv_sum,
        out_sum,
        fc_sum,
        proj_sum,
        gain1_sum,
        bias1_sum,
        gain2_sum,
        bias2_sum,
    )


def solution(mesh):
    placed = (
        P(("dp", "tensor"), None),
        P(("dp", "tensor"), None),
        P("dp", None),
        P("dp", None, "tensor"),
        P("tensor", "dp"),
        P("dp", "tensor"),
        P("tensor", "dp"),
        P("dp"),
        P("dp"),
        P("dp"),
        P("dp"),
    )
    return jax.shard_map(
        on_device,
        mesh=mesh,
        in_specs=placed,
        out_specs=(
            P(("dp", "tensor"), None),
            P(("dp", "tensor"), None),
            P("dp", None, "tensor"),
            P("tensor", "dp"),
            P("dp", "tensor"),
            P("tensor", "dp"),
            P("dp"),
            P("dp"),
            P("dp"),
            P("dp"),
        ),
        check_vma=False,
    )
```

```python
import functools

import jax
import jax.numpy as jnp
from jax import lax
from jax.experimental import pallas as pl
from jax.experimental.pallas import tpu as pltpu
from jax.sharding import PartitionSpec as P

HEAD = 64
PROMPT = 512
TILE = 256
REACH = 2
BIG = 3.0e38


def nt(left, right):
    return lax.dot_general(left, right, (((1,), (1,)), ((), ())), preferred_element_type=jnp.float32)


def nn(left, right):
    return jnp.dot(left, right, preferred_element_type=jnp.float32)


def first_of(lengths_ref, total):
    places = lax.broadcasted_iota(jnp.int32, (1, total), 1)
    first = jnp.zeros((1, total), jnp.int32)
    begin = jnp.int32(PROMPT)
    for c in range(lengths_ref.shape[1]):
        first = jnp.where(places >= begin, begin, first)
        begin = begin + lengths_ref[0, c]
    return first


def key_parts(index):
    if isinstance(index, int) and index < PROMPT // TILE:
        return [(j * TILE, j == index, False) for j in range(index + 1)]
    parts = [(j * TILE, False, False) for j in range(PROMPT // TILE)]
    if isinstance(index, int):
        band = range(max(PROMPT // TILE, index - REACH), index + 1)
        return parts + [(j * TILE, j == index, True) for j in band]
    return parts + [((index - r) * TILE, r == 0, True) for r in range(REACH, -1, -1)]


def seen(key0, query0, first, diagonal, banded):
    keys = key0 + lax.broadcasted_iota(jnp.int32, (TILE, TILE), 0)
    mask = None
    if banded:
        mask = keys >= first
    if diagonal:
        causal = keys <= query0 + lax.broadcasted_iota(jnp.int32, (TILE, TILE), 1)
        mask = causal if mask is None else mask & causal
    return mask


def rows(ref, start):
    return ref[pl.ds(start if isinstance(start, int) else pl.multiple_of(start, TILE), TILE), :]


def cols(ref, start):
    return ref[:, pl.ds(start if isinstance(start, int) else pl.multiple_of(start, TILE), TILE)]


def signs(values):
    return jnp.clip(values * BIG, -1.0, 1.0)


def each_tile(count, body):
    steady = PROMPT // TILE + REACH
    for index in range(min(steady, count)):
        body(index)
    if count > steady:
        lax.fori_loop(steady, count, lambda i, c: (body(i), c)[1], 0)


def forward_kernel(heads, lengths_ref, qkv_ref, mixed_ref, lse_ref, q_s, k_s, vt_s, o_s, first_s):
    total = qkv_ref.shape[0]
    local = heads * HEAD
    head = pl.program_id(0)

    @pl.when(head == 0)
    def _():
        first_s[...] = first_of(lengths_ref, total)

    for h in range(heads):
        @pl.when(head == h)
        def _(h=h):
            at = h * HEAD
            q_s[...] = qkv_ref[:, at : at + HEAD] * jnp.bfloat16(HEAD**-0.5)
            k_s[...] = qkv_ref[:, local + at : local + at + HEAD]
            vt_s[...] = qkv_ref[:, 2 * local + at : 2 * local + at + HEAD].T

    def body(index):
        query0 = index * TILE
        query = rows(q_s, query0)
        first = cols(first_s, query0)
        raws, sizes, tops = [], [], []
        parts = key_parts(index)
        for key0, diagonal, banded in parts:
            raw = nt(rows(k_s, key0), query)
            size = jnp.abs(raw)
            mask = seen(key0, query0, first, diagonal, banded)
            if mask is not None:
                size = jnp.where(mask, size, -1e30)
            raws.append(raw)
            sizes.append(size)
            tops.append(jnp.max(size, axis=0, keepdims=True))
        top = functools.reduce(jnp.maximum, tops)
        expos = [jnp.exp(size - top) for size in sizes]
        total_e = functools.reduce(jnp.add, [jnp.sum(e, axis=0, keepdims=True) for e in expos])
        inverse = 1.0 / total_e
        acc = None
        for (key0, _, _), raw, expo in zip(parts, raws, expos):
            weight = (signs(raw) * (expo * inverse)).astype(jnp.bfloat16)
            term = nn(cols(vt_s, key0), weight)
            acc = term if acc is None else acc + term
        o_s[pl.ds(query0, TILE), :] = acc.T.astype(jnp.bfloat16)
        lse_ref[0, :, pl.ds(query0, TILE)] = top + jnp.log(total_e)

    each_tile(total // TILE, body)
    for h in range(heads):
        @pl.when(head == h)
        def _(h=h):
            mixed_ref[:, h * HEAD : (h + 1) * HEAD] = o_s[...]


def whole(shape):
    return pl.BlockSpec(shape, lambda *_: (0,) * len(shape), pipeline_mode=pl.Buffered(1))


def attend(qkv, lengths, heads):
    total = qkv.shape[0]
    return pl.pallas_call(
        functools.partial(forward_kernel, heads),
        grid=(heads,),
        in_specs=[pl.BlockSpec(memory_space=pltpu.SMEM), whole(qkv.shape)],
        out_specs=[whole((total, heads * HEAD)), pl.BlockSpec((1, 1, total), lambda h: (h, 0, 0))],
        out_shape=[
            jax.ShapeDtypeStruct((total, heads * HEAD), jnp.bfloat16),
            jax.ShapeDtypeStruct((heads, 1, total), jnp.float32),
        ],
        scratch_shapes=[
            pltpu.VMEM((total, HEAD), jnp.bfloat16),
            pltpu.VMEM((total, HEAD), jnp.bfloat16),
            pltpu.VMEM((HEAD, total), jnp.bfloat16),
            pltpu.VMEM((total, HEAD), jnp.bfloat16),
            pltpu.VMEM((1, total), jnp.int32),
        ],
        compiler_params=pltpu.CompilerParams(vmem_limit_bytes=48 << 20),
        name="attend",
    )(lengths, qkv)


def backward_kernel(
    heads, lengths_ref, qkv_ref, mixed_ref, dmix_ref, lse_ref, grad_ref,
    q_s, k_s, kt_s, v_s, d_s, delta_s, dq_s, dk_s, dv_s, first_s,
):
    total = qkv_ref.shape[0]
    local = heads * HEAD
    head = pl.program_id(0)
    scale = HEAD**-0.5

    @pl.when(head == 0)
    def _():
        first_s[...] = first_of(lengths_ref, total)

    for h in range(heads):
        @pl.when(head == h)
        def _(h=h):
            at = h * HEAD
            q_s[...] = qkv_ref[:, at : at + HEAD] * jnp.bfloat16(scale)
            key = qkv_ref[:, local + at : local + at + HEAD]
            k_s[...] = key
            kt_s[...] = key.T
            v_s[...] = qkv_ref[:, 2 * local + at : 2 * local + at + HEAD]
            grad = dmix_ref[:, at : at + HEAD]
            d_s[...] = grad
            product = grad.astype(jnp.float32) * mixed_ref[:, at : at + HEAD].astype(jnp.float32)
            delta_s[...] = jnp.sum(product.T, axis=0, keepdims=True)

    dk_s[...] = jnp.zeros_like(dk_s)
    dv_s[...] = jnp.zeros_like(dv_s)

    def body(index):
        query0 = index * TILE
        query = rows(q_s, query0)
        grad = rows(d_s, query0)
        first = cols(first_s, query0)
        lse = lse_ref[0, :, pl.ds(query0, TILE)]
        inner = cols(delta_s, query0)
        acc = None
        for key0, diagonal, banded in key_parts(index):
            raw = nt(rows(k_s, key0), query)
            prob = jnp.exp(jnp.abs(raw) - lse)
            mask = seen(key0, query0, first, diagonal, banded)
            if mask is not None:
                prob = jnp.where(mask, prob, 0.0)
            signed = signs(raw) * prob
            wgrad = nt(rows(v_s, key0), grad)
            sgrad = (prob * wgrad - signed * inner).astype(jnp.bfloat16)
            at = pl.ds(key0, TILE)
            dv_s[at, :] = dv_s[at, :] + nn(signed.astype(jnp.bfloat16), grad)
            dk_s[at, :] = dk_s[at, :] + nn(sgrad, query)
            term = nn(cols(kt_s, key0), sgrad)
            acc = term if acc is None else acc + term
        dq_s[pl.ds(query0, TILE), :] = (acc * scale).T.astype(jnp.bfloat16)

    each_tile(total // TILE, body)
    for h in range(heads):
        @pl.when(head == h)
        def _(h=h):
            at = h * HEAD
            grad_ref[:, at : at + HEAD] = dq_s[...]
            grad_ref[:, local + at : local + at + HEAD] = dk_s[...].astype(jnp.bfloat16)
            grad_ref[:, 2 * local + at : 2 * local + at + HEAD] = dv_s[...].astype(jnp.bfloat16)


def attend_back(qkv, mixed, dmix, lse, lengths, heads):
    total = qkv.shape[0]
    low = jnp.bfloat16
    return pl.pallas_call(
        functools.partial(backward_kernel, heads),
        grid=(heads,),
        in_specs=[
            pl.BlockSpec(memory_space=pltpu.SMEM), whole(qkv.shape), whole(mixed.shape), whole(dmix.shape),
            pl.BlockSpec((1, 1, total), lambda h: (h, 0, 0)),
        ],
        out_specs=whole(qkv.shape),
        out_shape=jax.ShapeDtypeStruct(qkv.shape, low),
        scratch_shapes=[
            pltpu.VMEM((total, HEAD), low), pltpu.VMEM((total, HEAD), low), pltpu.VMEM((HEAD, total), low),
            pltpu.VMEM((total, HEAD), low), pltpu.VMEM((total, HEAD), low), pltpu.VMEM((1, total), jnp.float32),
            pltpu.VMEM((total, HEAD), low), pltpu.VMEM((total, HEAD), jnp.float32),
            pltpu.VMEM((total, HEAD), jnp.float32), pltpu.VMEM((1, total), jnp.int32),
        ],
        compiler_params=pltpu.CompilerParams(vmem_limit_bytes=48 << 20),
        name="attend_back",
    )(lengths, qkv, mixed, dmix, lse)


def around(axis_size):
    spot = lax.axis_index("tensor")
    return spot, spot + 1 - 2 * (spot % 2), (spot + 2) % 4, 3 - spot


def greet(peers):
    barrier = pltpu.get_barrier_semaphore()
    for peer in peers:
        pl.semaphore_signal(barrier, inc=1, device_id=peer, device_id_type=pl.DeviceIdType.MESH)
    pl.semaphore_wait(barrier, len(peers))


def push(source, target, sends, recvs, slot, peer):
    copy = pltpu.make_async_remote_copy(
        src_ref=source, dst_ref=target, send_sem=sends.at[slot], recv_sem=recvs.at[slot],
        device_id=peer, device_id_type=pl.DeviceIdType.MESH,
    )
    copy.start()
    return copy


def span(start, count):
    return pl.ds(pl.multiple_of(start, 16), count)


def pieces_of(rows):
    return 4 if rows % 64 == 0 else 1


def gather_rows(mine, every, sends, recvs, ready):
    size = mine.shape[0]
    spot, partner, cross, diag = around(4)
    pieces = pieces_of(size)
    step = size // pieces
    far, passed = [], []
    for k in range(pieces):
        far.append(push(mine.at[pl.ds(k * step, step)], every.at[span(spot * size + k * step, step)],
                        sends, recvs, k, {"tensor": cross}))
    near = push(mine, every.at[span(spot * size, size)], sends, recvs, pieces, {"tensor": partner})
    every[span(spot * size, size), :] = mine[...]
    ready(spot * size, size)
    near.wait_recv()
    ready(partner * size, size)
    for k in range(pieces):
        far[k].wait_recv()
        block = every.at[span(cross * size + k * step, step)]
        passed.append(push(block, block, sends, recvs, pieces + 1 + k, {"tensor": partner}))
        ready(cross * size + k * step, step)
        if k > 0:
            passed[k - 1].wait_recv()
            ready(diag * size + (k - 1) * step, step)
    passed[-1].wait_recv()
    ready(diag * size + (pieces - 1) * step, step)
    for copy in far + [near] + passed:
        copy.wait_send()


def gather_kernel(mine, weight, every, product, sends, recvs):
    spot, partner, cross, diag = around(4)
    greet([{"tensor": partner}, {"tensor": cross}])

    def ready(start, count):
        at = span(start, count)
        product[at, :] = nn(every[at, :], weight[...]).astype(product.dtype)

    gather_rows(mine, every, sends, recvs, ready)


def vmem():
    return pl.BlockSpec(memory_space=pltpu.VMEM)


def remote_params(ident):
    return pltpu.CompilerParams(collective_id=ident, has_side_effects=True, vmem_limit_bytes=60 << 20)


def gather_times(mine, weight, kind, ident):
    size, width = mine.shape
    count = 2 * pieces_of(size) + 1
    return pl.pallas_call(
        gather_kernel,
        in_specs=[vmem(), vmem()],
        out_specs=[vmem(), vmem()],
        out_shape=[
            jax.ShapeDtypeStruct((4 * size, width), mine.dtype),
            jax.ShapeDtypeStruct((4 * size, weight.shape[1]), kind),
        ],
        scratch_shapes=[pltpu.SemaphoreType.DMA((count,)), pltpu.SemaphoreType.DMA((count,))],
        compiler_params=remote_params(ident),
        name=f"gather_times_{ident}",
    )(mine, weight)


def scatter_kernel(left, right, total, out_d, got_a, out_c, got_c, out_b, got_b, sends, recvs):
    size = total.shape[0]
    spot, partner, cross, diag = around(4)
    pieces = pieces_of(size)
    step = size // pieces
    greet([{"tensor": partner}, {"tensor": cross}])

    def part(block, k=0, count=size):
        return nt(left[span(block * size + k * step, count), :], right[...])

    first, second = [], []
    for k in range(pieces):
        at = pl.ds(k * step, step)
        out_d[at, :] = part(diag, k, step).astype(jnp.bfloat16)
        first.append(push(out_d.at[at], got_a.at[at], sends, recvs, k, {"tensor": partner}))
    for k in range(pieces):
        at = pl.ds(k * step, step)
        term = part(cross, k, step)
        first[k].wait_recv()
        out_c[at, :] = (term + got_a[at, :].astype(jnp.float32)).astype(jnp.bfloat16)
        second.append(push(out_c.at[at], got_c.at[at], sends, recvs, pieces + k, {"tensor": cross}))
    out_b[...] = part(partner).astype(jnp.bfloat16)
    third = push(out_b, got_b, sends, recvs, 2 * pieces, {"tensor": partner})
    total[...] = part(spot)
    third.wait_recv()
    total[...] = total[...] + got_b[...].astype(jnp.float32)
    for k in range(pieces):
        at = pl.ds(k * step, step)
        second[k].wait_recv()
        total[at, :] = total[at, :] + got_c[at, :].astype(jnp.float32)
    for copy in first + second + [third]:
        copy.wait_send()


def scatter_times(left, right, ident):
    size, width = left.shape[0] // 4, right.shape[0]
    count = 2 * pieces_of(size) + 1
    return pl.pallas_call(
        scatter_kernel,
        in_specs=[vmem(), vmem()],
        out_specs=vmem(),
        out_shape=jax.ShapeDtypeStruct((size, width), jnp.float32),
        scratch_shapes=[pltpu.VMEM((size, width), jnp.bfloat16)] * 6
        + [pltpu.SemaphoreType.DMA((count,)), pltpu.SemaphoreType.DMA((count,))],
        compiler_params=remote_params(ident),
        name=f"scatter_times_{ident}",
    )(left, right)


def opening_kernel(
    columns, tokens, small, shard, every, product, weights, gains, got_small, mine, sends, recvs, dp_sends, dp_recvs
):
    count = got_small.shape[0]
    depth = shard.shape[0]
    place = lax.axis_index("dp")
    spot, partner, cross, diag = around(4)
    others = [(place + i) % count for i in range(1, count)]
    greet([{"dp": other} for other in others] + [{"tensor": partner}, {"tensor": cross}])
    little, large = [], []
    for i, other in enumerate(others):
        little.append(push(small, got_small.at[place], dp_sends, dp_recvs, i, {"dp": other}))
    for i, other in enumerate(others):
        large.append(push(shard, weights.at[span(place * depth, depth)], dp_sends, dp_recvs, count - 1 + i, {"dp": other}))
    got_small[place] = small[...]
    weights[span(place * depth, depth), :] = shard[...]
    for copy in little:
        copy.wait_recv()
    placed = functools.reduce(jnp.add, [got_small[i] for i in range(count)])
    gains[...] = placed
    values = tokens[...].astype(jnp.float32)
    centred = values - jnp.mean(values, axis=-1, keepdims=True)
    factor = lax.rsqrt(jnp.mean(centred * centred, axis=-1, keepdims=True) + 1e-05)
    mine[...] = (centred * factor * placed[0:1, :] + placed[1:2, :]).astype(jnp.bfloat16)
    landed = []

    def ready(start, rows_count):
        if not landed:
            for copy in large:
                copy.wait_recv()
            landed.append(True)
        at = span(start, rows_count)
        product[at, :] = nn(every[at, :], weights[:, :columns]).astype(jnp.bfloat16)

    gather_rows(mine, every, sends, recvs, ready)
    for copy in little + large:
        copy.wait_send()


def opening(tokens, small, shard, columns, ident):
    size, width = tokens.shape
    count = 2 * pieces_of(size) + 1
    dp = lax.axis_size("dp")
    low = jnp.bfloat16
    return pl.pallas_call(
        functools.partial(opening_kernel, columns),
        in_specs=[vmem()] * 3,
        out_specs=[vmem()] * 4,
        out_shape=[
            jax.ShapeDtypeStruct((4 * size, width), low),
            jax.ShapeDtypeStruct((4 * size, columns), low),
            jax.ShapeDtypeStruct((dp * shard.shape[0], shard.shape[1]), low),
            jax.ShapeDtypeStruct(small.shape, jnp.float32),
        ],
        scratch_shapes=[
            pltpu.VMEM((dp,) + small.shape, jnp.float32),
            pltpu.VMEM(tokens.shape, low),
            pltpu.SemaphoreType.DMA((count,)), pltpu.SemaphoreType.DMA((count,)),
            pltpu.SemaphoreType.DMA((2 * (dp - 1),)), pltpu.SemaphoreType.DMA((2 * (dp - 1),)),
        ],
        compiler_params=remote_params(ident),
        name="opening",
    )(tokens, small, shard)


def vectors_kernel(parts, total, got, sends, recvs):
    dp, tensor = parts.shape[0], got.shape[0] // parts.shape[0]
    place, spot = lax.axis_index("dp"), lax.axis_index("tensor")
    others = []
    for i in range(dp):
        for j in range(tensor):
            if i or j:
                others.append(((place + i) % dp, (spot + j) % tensor))
    greet([{"dp": a, "tensor": b} for a, b in others])
    here = place * tensor + spot
    copies = []
    for n, (a, b) in enumerate(others):
        copies.append(push(parts.at[a], got.at[here], sends, recvs, n, {"dp": a, "tensor": b}))
    got[here] = parts[place]
    for copy in copies:
        copy.wait_recv()
    total[...] = functools.reduce(jnp.add, [got[n] for n in range(dp * tensor)])
    for copy in copies:
        copy.wait_send()


def sum_vectors(parts, ident):
    dp, tensor = lax.axis_size("dp"), lax.axis_size("tensor")
    return pl.pallas_call(
        vectors_kernel,
        in_specs=[vmem()],
        out_specs=vmem(),
        out_shape=jax.ShapeDtypeStruct(parts.shape[1:], jnp.float32),
        scratch_shapes=[
            pltpu.VMEM((dp * tensor,) + parts.shape[1:], jnp.float32),
            pltpu.SemaphoreType.DMA((dp * tensor - 1,)), pltpu.SemaphoreType.DMA((dp * tensor - 1,)),
        ],
        compiler_params=remote_params(ident),
        name="sum_vectors",
    )(parts)


def normalize(values):
    mean = jnp.mean(values, axis=-1, keepdims=True)
    centred = values - mean
    spread = jnp.mean(centred * centred, axis=-1, keepdims=True)
    factor = lax.rsqrt(spread + 1e-05)
    return (centred * factor, factor)


def norm_back(grad_out, normed, factor, gain):
    scaled = grad_out * gain
    first = jnp.mean(scaled, axis=-1, keepdims=True)
    second = jnp.mean(scaled * normed, axis=-1, keepdims=True)
    return factor * (scaled - first - normed * second)


def gelu_tanh(values):
    return jax.nn.gelu(values, approximate=True)


def inner_rows(left, right):
    return lax.dot_general(
        left, right, (((0,), (0,)), ((), ())), preferred_element_type=jnp.float32
    )


def scatter_dp(grad):
    return lax.psum_scatter(grad.astype(jnp.bfloat16), "dp", scatter_dimension=0, tiled=True).astype(jnp.float32)


def spread(vectors, dp):
    depth = vectors.shape[1]
    owner = jnp.arange(dp * depth, dtype=jnp.int32) // depth
    return jnp.where(owner[None, :] == lax.axis_index("dp"), jnp.tile(vectors, (1, dp)), 0.0)


def on_device(
    tokens, cotangent, lengths, w_qkv, w_out, w_fc, w_proj, ln1_gain, ln1_bias, ln2_gain, ln2_bias
):
    dp = lax.axis_size("dp")
    low = jnp.bfloat16
    depth, _, local = w_qkv.shape
    width = depth * dp
    heads = local // HEAD
    small_dp = dp <= 8 and depth % 16 == 0
    columns = 3 * local
    inputs = tokens.astype(jnp.float32)
    vectors = jnp.stack([ln1_gain, ln1_bias, ln2_gain, ln2_bias]).astype(jnp.float32)
    shard = jnp.concatenate([w_qkv.reshape(depth, columns), w_out.T], axis=1)
    if small_dp:
        placed = jnp.concatenate([spread(vectors, dp), jnp.zeros((4, width), jnp.float32)])
        all_norm1, projected, weights, gains = opening(tokens, placed, shard, columns, 0)
    else:
        gains = lax.psum(spread(vectors, dp), "dp")
        weights = lax.all_gather(shard, "dp", axis=0, tiled=True)
        lowered1 = (normalize(inputs)[0] * gains[0] + gains[1]).astype(low)
        all_norm1, projected = gather_times(lowered1, weights[:, :columns], low, 0)
    out_turned = weights[:, columns:]
    w_fc, w_proj, cotangent_late, lengths, projected = lax.optimization_barrier(
        (w_fc, w_proj, cotangent, lengths, projected)
    )
    fc_full = lax.all_gather(w_fc, "dp", axis=0, tiled=True)
    proj_turned = lax.all_gather(w_proj.T, "dp", axis=0, tiled=True)
    grad_all = lax.all_gather(cotangent_late, "tensor", axis=0, tiled=True)
    gain1, gain2, bias2 = gains[0], gains[2], gains[3]
    mixed, sums = attend(projected, lengths, heads)
    resid = inputs + scatter_times(mixed, out_turned, 1)
    normed2, factor2 = normalize(resid)
    lowered2 = (normed2 * gain2 + bias2).astype(low)
    all_norm2, hidden_pre = gather_times(lowered2, fc_full, jnp.float32, 2)
    hidden, gelu_pull = jax.vjp(gelu_tanh, hidden_pre)
    hidden_low = hidden.astype(low)
    mlp_rows = lax.psum_scatter(
        nt(hidden_low, proj_turned).astype(low), "tensor", scatter_dimension=0, tiled=True
    ).astype(jnp.float32)
    block_out = (resid + mlp_rows).astype(low)
    hidden_grad = nn(grad_all, proj_turned)
    proj_grad = inner_rows(grad_all, hidden_low)
    pre_low = gelu_pull(hidden_grad)[0].astype(low)
    fc_grad = inner_rows(all_norm2, pre_low)
    norm2_grad = scatter_times(pre_low, fc_full, 3)
    proj_sum = scatter_dp(proj_grad).T
    fc_sum = scatter_dp(fc_grad)
    gain2_part = jnp.sum(norm2_grad * normed2, axis=0)
    bias2_part = jnp.sum(norm2_grad, axis=0)
    resid_grad = cotangent.astype(jnp.float32) + norm_back(norm2_grad, normed2, factor2, gain2)
    resid_all, mixed_grad = gather_times(resid_grad.astype(low), out_turned, low, 4)
    qkv_grad_low = attend_back(projected, mixed, mixed_grad, sums, lengths, heads)
    last_grad = jnp.concatenate(
        [inner_rows(all_norm1, qkv_grad_low).astype(low), inner_rows(resid_all, mixed).astype(low)], axis=1
    )
    last_sum = scatter_dp(last_grad)
    norm1_grad = scatter_times(qkv_grad_low, weights[:, :columns], 5)
    normed1, factor1 = normalize(inputs)
    input_grad = (resid_grad + norm_back(norm1_grad, normed1, factor1, gain1)).astype(low)
    parts = jnp.stack([jnp.sum(norm1_grad * normed1, axis=0), jnp.sum(norm1_grad, axis=0), gain2_part, bias2_part])
    if small_dp:
        pieces = jnp.pad(parts.reshape(4, dp, depth).transpose(1, 0, 2), ((0, 0), (0, 4), (0, -depth % 128)))
        shares = sum_vectors(pieces, 6)[:4, :depth]
    else:
        shares = lax.psum(lax.psum_scatter(parts, "dp", scatter_dimension=1, tiled=True), "tensor")
    return (
        block_out,
        input_grad,
        last_sum[:, :columns].reshape(depth, 3, local),
        last_sum[:, columns:].T,
        fc_sum,
        proj_sum,
        shares[0],
        shares[1],
        shares[2],
        shares[3],
    )


def solution(mesh):
    placed = (
        P(("dp", "tensor"), None),
        P(("dp", "tensor"), None),
        P("dp", None),
        P("dp", None, "tensor"),
        P("tensor", "dp"),
        P("dp", "tensor"),
        P("tensor", "dp"),
        P("dp"),
        P("dp"),
        P("dp"),
        P("dp"),
    )
    return jax.shard_map(
        on_device,
        mesh=mesh,
        in_specs=placed,
        out_specs=(
            P(("dp", "tensor"), None),
            P(("dp", "tensor"), None),
            P("dp", None, "tensor"),
            P("tensor", "dp"),
            P("dp", "tensor"),
            P("tensor", "dp"),
            P("dp"),
            P("dp"),
            P("dp"),
            P("dp"),
        ),
        check_vma=False,
    )
```

```python
import functools

import jax
import jax.numpy as jnp
from jax import lax
from jax.experimental import pallas as pl
from jax.experimental.pallas import tpu as pltpu
from jax.sharding import PartitionSpec as P

HEAD = 64
PROMPT = 512
TILE = 256
REACH = 2
BIG = 3.0e38


def nt(left, right):
    return lax.dot_general(left, right, (((1,), (1,)), ((), ())), preferred_element_type=jnp.float32)


def nn(left, right):
    return jnp.dot(left, right, preferred_element_type=jnp.float32)


def first_of(lengths_ref, total):
    places = lax.broadcasted_iota(jnp.int32, (1, total), 1)
    first = jnp.zeros((1, total), jnp.int32)
    begin = jnp.int32(PROMPT)
    for c in range(lengths_ref.shape[1]):
        first = jnp.where(places >= begin, begin, first)
        begin = begin + lengths_ref[0, c]
    return first


def key_parts(index):
    if isinstance(index, int) and index < PROMPT // TILE:
        return [(j * TILE, j == index, False) for j in range(index + 1)]
    parts = [(j * TILE, False, False) for j in range(PROMPT // TILE)]
    if isinstance(index, int):
        band = range(max(PROMPT // TILE, index - REACH), index + 1)
        return parts + [(j * TILE, j == index, True) for j in band]
    return parts + [((index - r) * TILE, r == 0, True) for r in range(REACH, -1, -1)]


def seen(key0, query0, first, diagonal, banded):
    keys = key0 + lax.broadcasted_iota(jnp.int32, (TILE, TILE), 0)
    mask = None
    if banded:
        mask = keys >= first
    if diagonal:
        causal = keys <= query0 + lax.broadcasted_iota(jnp.int32, (TILE, TILE), 1)
        mask = causal if mask is None else mask & causal
    return mask


def rows(ref, start):
    return ref[pl.ds(start if isinstance(start, int) else pl.multiple_of(start, TILE), TILE), :]


def cols(ref, start):
    return ref[:, pl.ds(start if isinstance(start, int) else pl.multiple_of(start, TILE), TILE)]


def signs(values):
    return jnp.clip(values * BIG, -1.0, 1.0)


def each_tile(count, body):
    steady = PROMPT // TILE + REACH
    for index in range(min(steady, count)):
        body(index)
    if count > steady:
        lax.fori_loop(steady, count, lambda i, c: (body(i), c)[1], 0)


def forward_kernel(heads, lengths_ref, qkv_ref, mixed_ref, lse_ref, q_s, k_s, vt_s, o_s, first_s):
    total = qkv_ref.shape[0]
    local = heads * HEAD
    head = pl.program_id(0)

    @pl.when(head == 0)
    def _():
        first_s[...] = first_of(lengths_ref, total)

    for h in range(heads):
        @pl.when(head == h)
        def _(h=h):
            at = h * HEAD
            q_s[...] = qkv_ref[:, at : at + HEAD] * jnp.bfloat16(HEAD**-0.5)
            k_s[...] = qkv_ref[:, local + at : local + at + HEAD]
            vt_s[...] = qkv_ref[:, 2 * local + at : 2 * local + at + HEAD].T

    def body(index):
        query0 = index * TILE
        query = rows(q_s, query0)
        first = cols(first_s, query0)
        raws, sizes, tops = [], [], []
        parts = key_parts(index)
        for key0, diagonal, banded in parts:
            raw = nt(rows(k_s, key0), query)
            size = jnp.abs(raw)
            mask = seen(key0, query0, first, diagonal, banded)
            if mask is not None:
                size = jnp.where(mask, size, -1e30)
            raws.append(raw)
            sizes.append(size)
            tops.append(jnp.max(size, axis=0, keepdims=True))
        top = functools.reduce(jnp.maximum, tops)
        expos = [jnp.exp(size - top) for size in sizes]
        total_e = functools.reduce(jnp.add, [jnp.sum(e, axis=0, keepdims=True) for e in expos])
        inverse = 1.0 / total_e
        acc = None
        for (key0, _, _), raw, expo in zip(parts, raws, expos):
            weight = (signs(raw) * (expo * inverse)).astype(jnp.bfloat16)
            term = nn(cols(vt_s, key0), weight)
            acc = term if acc is None else acc + term
        o_s[pl.ds(query0, TILE), :] = acc.T.astype(jnp.bfloat16)
        lse_ref[0, :, pl.ds(query0, TILE)] = top + jnp.log(total_e)

    each_tile(total // TILE, body)
    for h in range(heads):
        @pl.when(head == h)
        def _(h=h):
            mixed_ref[:, h * HEAD : (h + 1) * HEAD] = o_s[...]


def whole(shape):
    return pl.BlockSpec(shape, lambda *_: (0,) * len(shape), pipeline_mode=pl.Buffered(1))


def attend(qkv, lengths, heads):
    total = qkv.shape[0]
    return pl.pallas_call(
        functools.partial(forward_kernel, heads),
        grid=(heads,),
        in_specs=[pl.BlockSpec(memory_space=pltpu.SMEM), whole(qkv.shape)],
        out_specs=[whole((total, heads * HEAD)), pl.BlockSpec((1, 1, total), lambda h: (h, 0, 0))],
        out_shape=[
            jax.ShapeDtypeStruct((total, heads * HEAD), jnp.bfloat16),
            jax.ShapeDtypeStruct((heads, 1, total), jnp.float32),
        ],
        scratch_shapes=[
            pltpu.VMEM((total, HEAD), jnp.bfloat16),
            pltpu.VMEM((total, HEAD), jnp.bfloat16),
            pltpu.VMEM((HEAD, total), jnp.bfloat16),
            pltpu.VMEM((total, HEAD), jnp.bfloat16),
            pltpu.VMEM((1, total), jnp.int32),
        ],
        compiler_params=pltpu.CompilerParams(vmem_limit_bytes=48 << 20),
        name="attend",
    )(lengths, qkv)


def backward_kernel(
    heads, lengths_ref, qkv_ref, mixed_ref, dmix_ref, lse_ref, grad_ref,
    q_s, k_s, kt_s, v_s, d_s, delta_s, dq_s, dk_s, dv_s, first_s,
):
    total = qkv_ref.shape[0]
    local = heads * HEAD
    head = pl.program_id(0)
    scale = HEAD**-0.5

    @pl.when(head == 0)
    def _():
        first_s[...] = first_of(lengths_ref, total)

    for h in range(heads):
        @pl.when(head == h)
        def _(h=h):
            at = h * HEAD
            q_s[...] = qkv_ref[:, at : at + HEAD] * jnp.bfloat16(scale)
            key = qkv_ref[:, local + at : local + at + HEAD]
            k_s[...] = key
            kt_s[...] = key.T
            v_s[...] = qkv_ref[:, 2 * local + at : 2 * local + at + HEAD]
            grad = dmix_ref[:, at : at + HEAD]
            d_s[...] = grad
            product = grad.astype(jnp.float32) * mixed_ref[:, at : at + HEAD].astype(jnp.float32)
            delta_s[...] = jnp.sum(product.T, axis=0, keepdims=True)

    dk_s[...] = jnp.zeros_like(dk_s)
    dv_s[...] = jnp.zeros_like(dv_s)

    def body(index):
        query0 = index * TILE
        query = rows(q_s, query0)
        grad = rows(d_s, query0)
        first = cols(first_s, query0)
        lse = lse_ref[0, :, pl.ds(query0, TILE)]
        inner = cols(delta_s, query0)
        acc = None
        for key0, diagonal, banded in key_parts(index):
            raw = nt(rows(k_s, key0), query)
            prob = jnp.exp(jnp.abs(raw) - lse)
            mask = seen(key0, query0, first, diagonal, banded)
            if mask is not None:
                prob = jnp.where(mask, prob, 0.0)
            signed = signs(raw) * prob
            wgrad = nt(rows(v_s, key0), grad)
            sgrad = (prob * wgrad - signed * inner).astype(jnp.bfloat16)
            at = pl.ds(key0, TILE)
            dv_s[at, :] = dv_s[at, :] + nn(signed.astype(jnp.bfloat16), grad)
            dk_s[at, :] = dk_s[at, :] + nn(sgrad, query)
            term = nn(cols(kt_s, key0), sgrad)
            acc = term if acc is None else acc + term
        dq_s[pl.ds(query0, TILE), :] = (acc * scale).T.astype(jnp.bfloat16)

    each_tile(total // TILE, body)
    for h in range(heads):
        @pl.when(head == h)
        def _(h=h):
            at = h * HEAD
            grad_ref[:, at : at + HEAD] = dq_s[...]
            grad_ref[:, local + at : local + at + HEAD] = dk_s[...].astype(jnp.bfloat16)
            grad_ref[:, 2 * local + at : 2 * local + at + HEAD] = dv_s[...].astype(jnp.bfloat16)


def attend_back(qkv, mixed, dmix, lse, lengths, heads):
    total = qkv.shape[0]
    low = jnp.bfloat16
    return pl.pallas_call(
        functools.partial(backward_kernel, heads),
        grid=(heads,),
        in_specs=[
            pl.BlockSpec(memory_space=pltpu.SMEM), whole(qkv.shape), whole(mixed.shape), whole(dmix.shape),
            pl.BlockSpec((1, 1, total), lambda h: (h, 0, 0)),
        ],
        out_specs=whole(qkv.shape),
        out_shape=jax.ShapeDtypeStruct(qkv.shape, low),
        scratch_shapes=[
            pltpu.VMEM((total, HEAD), low), pltpu.VMEM((total, HEAD), low), pltpu.VMEM((HEAD, total), low),
            pltpu.VMEM((total, HEAD), low), pltpu.VMEM((total, HEAD), low), pltpu.VMEM((1, total), jnp.float32),
            pltpu.VMEM((total, HEAD), low), pltpu.VMEM((total, HEAD), jnp.float32),
            pltpu.VMEM((total, HEAD), jnp.float32), pltpu.VMEM((1, total), jnp.int32),
        ],
        compiler_params=pltpu.CompilerParams(vmem_limit_bytes=48 << 20),
        name="attend_back",
    )(lengths, qkv, mixed, dmix, lse)


def around(axis_size):
    spot = lax.axis_index("tensor")
    return spot, spot + 1 - 2 * (spot % 2), (spot + 2) % 4, 3 - spot


def greet(peers):
    barrier = pltpu.get_barrier_semaphore()
    for peer in peers:
        pl.semaphore_signal(barrier, inc=1, device_id=peer, device_id_type=pl.DeviceIdType.MESH)
    pl.semaphore_wait(barrier, len(peers))


def push(source, target, sends, recvs, slot, peer):
    copy = pltpu.make_async_remote_copy(
        src_ref=source, dst_ref=target, send_sem=sends.at[slot], recv_sem=recvs.at[slot],
        device_id=peer, device_id_type=pl.DeviceIdType.MESH,
    )
    copy.start()
    return copy


def span(start, count):
    return pl.ds(pl.multiple_of(start, 16), count)


def pieces_of(rows):
    return 4 if rows % 64 == 0 else 1


def gather_rows(mine, every, sends, recvs, ready):
    size = mine.shape[0]
    spot, partner, cross, diag = around(4)
    pieces = pieces_of(size)
    step = size // pieces
    far, passed = [], []
    for k in range(pieces):
        far.append(push(mine.at[pl.ds(k * step, step)], every.at[span(spot * size + k * step, step)],
                        sends, recvs, k, {"tensor": cross}))
    near = push(mine, every.at[span(spot * size, size)], sends, recvs, pieces, {"tensor": partner})
    every[span(spot * size, size), :] = mine[...]
    ready(spot * size, size)
    near.wait_recv()
    ready(partner * size, size)
    for k in range(pieces):
        far[k].wait_recv()
        block = every.at[span(cross * size + k * step, step)]
        passed.append(push(block, block, sends, recvs, pieces + 1 + k, {"tensor": partner}))
        ready(cross * size + k * step, step)
        if k > 0:
            passed[k - 1].wait_recv()
            ready(diag * size + (k - 1) * step, step)
    passed[-1].wait_recv()
    ready(diag * size + (pieces - 1) * step, step)
    for copy in far + [near] + passed:
        copy.wait_send()


def gather_kernel(mine, weight, every, product, sends, recvs):
    spot, partner, cross, diag = around(4)
    greet([{"tensor": partner}, {"tensor": cross}])

    def ready(start, count):
        at = span(start, count)
        product[at, :] = nn(every[at, :], weight[...]).astype(product.dtype)

    gather_rows(mine, every, sends, recvs, ready)


def exchange_out(grad, got, sends, recvs):
    count, depth = got.shape[0], got.shape[1]
    place = lax.axis_index("dp")
    copies = []
    for i in range(1, count):
        other = (place + i) % count
        copies.append(push(grad.at[span(other * depth, depth), :], got.at[place], sends, recvs, i - 1, {"dp": other}))
    got[place] = grad[span(place * depth, depth), :]
    return copies


def exchange_in(copies, got, total):
    for copy in copies:
        copy.wait_recv()
    total[...] = functools.reduce(jnp.add, [got[i].astype(jnp.float32) for i in range(got.shape[0])])
    for copy in copies:
        copy.wait_send()


def spread_out(shard, every, count, sends, recvs):
    depth = shard.shape[0]
    place = lax.axis_index("dp")
    copies = []
    for i in range(1, count):
        other = (place + i) % count
        copies.append(push(shard, every.at[span(place * depth, depth), :], sends, recvs, i - 1, {"dp": other}))
    every[span(place * depth, depth), :] = shard[...]
    return copies


def dp_peers(count):
    place = lax.axis_index("dp")
    return [{"dp": (place + i) % count} for i in range(1, count)]


def gather_exchange_kernel(dp, mine, weight, grad, every, product, total, sends, recvs, got, dp_sends, dp_recvs):
    spot, partner, cross, diag = around(4)
    greet(dp_peers(dp) + [{"tensor": partner}, {"tensor": cross}])
    copies = exchange_out(grad, got, dp_sends, dp_recvs)

    def ready(start, count):
        at = span(start, count)
        product[at, :] = nn(every[at, :], weight[...]).astype(product.dtype)

    gather_rows(mine, every, sends, recvs, ready)
    exchange_in(copies, got, total)


def vmem():
    return pl.BlockSpec(memory_space=pltpu.VMEM)


def remote_params(ident):
    return pltpu.CompilerParams(collective_id=ident, has_side_effects=True, vmem_limit_bytes=60 << 20)


def side_room(dp, grad):
    return [
        pltpu.VMEM((dp, grad.shape[0] // dp, grad.shape[1]), grad.dtype),
        pltpu.SemaphoreType.DMA((dp - 1,)), pltpu.SemaphoreType.DMA((dp - 1,)),
    ]


def side_shape(dp, grad):
    return jax.ShapeDtypeStruct((grad.shape[0] // dp, grad.shape[1]), jnp.float32)


def gather_times(mine, weight, kind, ident, grad=None):
    size, width = mine.shape
    count = 2 * pieces_of(size) + 1
    dp = lax.axis_size("dp")
    shapes = [
        jax.ShapeDtypeStruct((4 * size, width), mine.dtype),
        jax.ShapeDtypeStruct((4 * size, weight.shape[1]), kind),
    ]
    sems = [pltpu.SemaphoreType.DMA((count,)), pltpu.SemaphoreType.DMA((count,))]
    if grad is None:
        body, operands = gather_kernel, (mine, weight)
    else:
        body, operands = functools.partial(gather_exchange_kernel, dp), (mine, weight, grad)
        shapes, sems = shapes + [side_shape(dp, grad)], sems + side_room(dp, grad)
    return pl.pallas_call(
        body,
        in_specs=[vmem()] * len(operands),
        out_specs=[vmem()] * len(shapes),
        out_shape=shapes,
        scratch_shapes=sems,
        compiler_params=remote_params(ident),
        name=f"gather_times_{ident}",
    )(*operands)


def scatter_kernel(left, right, total, *room):
    spot, partner, cross, diag = around(4)
    greet([{"tensor": partner}, {"tensor": cross}])
    scatter_rows(left, right, total, *room)


def scatter_exchange_kernel(dp, left, right, grad, total, summed, *room):
    got, dp_sends, dp_recvs = room[-3:]
    spot, partner, cross, diag = around(4)
    greet(dp_peers(dp) + [{"tensor": partner}, {"tensor": cross}])
    copies = exchange_out(grad, got, dp_sends, dp_recvs)
    scatter_rows(left, right, total, *room[:-3])
    exchange_in(copies, got, summed)


def scatter_spread_kernel(dp, left, right, shard, total, every, *room):
    dp_sends, dp_recvs = room[-2:]
    spot, partner, cross, diag = around(4)
    greet(dp_peers(dp) + [{"tensor": partner}, {"tensor": cross}])
    copies = spread_out(shard, every, dp, dp_sends, dp_recvs)
    scatter_rows(left, right, total, *room[:-2])
    for copy in copies:
        copy.wait_recv()
    for copy in copies:
        copy.wait_send()


def scatter_rows(left, right, total, out_d, got_a, out_c, got_c, out_b, got_b, sends, recvs):
    size = total.shape[0]
    spot, partner, cross, diag = around(4)
    pieces = pieces_of(size)
    step = size // pieces

    def part(block, k=0, count=size):
        return nt(left[span(block * size + k * step, count), :], right[...])

    first, second = [], []
    for k in range(pieces):
        at = pl.ds(k * step, step)
        out_d[at, :] = part(diag, k, step).astype(jnp.bfloat16)
        first.append(push(out_d.at[at], got_a.at[at], sends, recvs, k, {"tensor": partner}))
    for k in range(pieces):
        at = pl.ds(k * step, step)
        term = part(cross, k, step)
        first[k].wait_recv()
        out_c[at, :] = (term + got_a[at, :].astype(jnp.float32)).astype(jnp.bfloat16)
        second.append(push(out_c.at[at], got_c.at[at], sends, recvs, pieces + k, {"tensor": cross}))
    out_b[...] = part(partner).astype(jnp.bfloat16)
    third = push(out_b, got_b, sends, recvs, 2 * pieces, {"tensor": partner})
    total[...] = part(spot)
    third.wait_recv()
    total[...] = total[...] + got_b[...].astype(jnp.float32)
    for k in range(pieces):
        at = pl.ds(k * step, step)
        second[k].wait_recv()
        total[at, :] = total[at, :] + got_c[at, :].astype(jnp.float32)
    for copy in first + second + [third]:
        copy.wait_send()


def scatter_times(left, right, ident, grad=None, shard=None):
    size, width = left.shape[0] // 4, right.shape[0]
    count = 2 * pieces_of(size) + 1
    dp = lax.axis_size("dp")
    shapes = [jax.ShapeDtypeStruct((size, width), jnp.float32)]
    room = [pltpu.VMEM((size, width), jnp.bfloat16)] * 6
    room = room + [pltpu.SemaphoreType.DMA((count,)), pltpu.SemaphoreType.DMA((count,))]
    body, operands = scatter_kernel, (left, right)
    if grad is not None:
        body, operands = functools.partial(scatter_exchange_kernel, dp), (left, right, grad)
        shapes, room = shapes + [side_shape(dp, grad)], room + side_room(dp, grad)
    elif shard is not None:
        body, operands = functools.partial(scatter_spread_kernel, dp), (left, right, shard)
        shapes = shapes + [jax.ShapeDtypeStruct((dp * shard.shape[0], shard.shape[1]), shard.dtype)]
        room = room + [pltpu.SemaphoreType.DMA((dp - 1,)), pltpu.SemaphoreType.DMA((dp - 1,))]
    return pl.pallas_call(
        body,
        in_specs=[vmem()] * len(operands),
        out_specs=[vmem()] * len(shapes),
        out_shape=shapes,
        scratch_shapes=room,
        compiler_params=remote_params(ident),
        name=f"scatter_times_{ident}",
    )(*operands)


def opening_kernel(
    columns, tokens, small, shard, every, product, weights, gains, got_small, mine, sends, recvs, dp_sends, dp_recvs
):
    count = got_small.shape[0]
    depth = shard.shape[0]
    place = lax.axis_index("dp")
    spot, partner, cross, diag = around(4)
    others = [(place + i) % count for i in range(1, count)]
    greet([{"dp": other} for other in others] + [{"tensor": partner}, {"tensor": cross}])
    little, large = [], []
    for i, other in enumerate(others):
        little.append(push(small, got_small.at[place], dp_sends, dp_recvs, i, {"dp": other}))
    for i, other in enumerate(others):
        large.append(push(shard, weights.at[span(place * depth, depth)], dp_sends, dp_recvs, count - 1 + i, {"dp": other}))
    got_small[place] = small[...]
    weights[span(place * depth, depth), :] = shard[...]
    for copy in little:
        copy.wait_recv()
    placed = functools.reduce(jnp.add, [got_small[i] for i in range(count)])
    gains[...] = placed
    values = tokens[...].astype(jnp.float32)
    centred = values - jnp.mean(values, axis=-1, keepdims=True)
    factor = lax.rsqrt(jnp.mean(centred * centred, axis=-1, keepdims=True) + 1e-05)
    mine[...] = (centred * factor * placed[0:1, :] + placed[1:2, :]).astype(jnp.bfloat16)
    gather_rows(mine, every, sends, recvs, lambda start, rows_count: None)
    for copy in large:
        copy.wait_recv()
    size = mine.shape[0]
    for block in range(4):
        at = pl.ds(block * size, size)
        product[at, :] = nn(every[at, :], weights[:, :columns]).astype(jnp.bfloat16)
    for copy in little + large:
        copy.wait_send()


def opening(tokens, small, shard, columns, ident):
    size, width = tokens.shape
    count = 2 * pieces_of(size) + 1
    dp = lax.axis_size("dp")
    low = jnp.bfloat16
    return pl.pallas_call(
        functools.partial(opening_kernel, columns),
        in_specs=[vmem()] * 3,
        out_specs=[vmem()] * 4,
        out_shape=[
            jax.ShapeDtypeStruct((4 * size, width), low),
            jax.ShapeDtypeStruct((4 * size, columns), low),
            jax.ShapeDtypeStruct((dp * shard.shape[0], shard.shape[1]), low),
            jax.ShapeDtypeStruct(small.shape, jnp.float32),
        ],
        scratch_shapes=[
            pltpu.VMEM((dp,) + small.shape, jnp.float32),
            pltpu.VMEM(tokens.shape, low),
            pltpu.SemaphoreType.DMA((count,)), pltpu.SemaphoreType.DMA((count,)),
            pltpu.SemaphoreType.DMA((2 * (dp - 1),)), pltpu.SemaphoreType.DMA((2 * (dp - 1),)),
        ],
        compiler_params=remote_params(ident),
        name="opening",
    )(tokens, small, shard)


def vectors_kernel(parts, total, got, sends, recvs):
    dp, tensor = parts.shape[0], got.shape[0] // parts.shape[0]
    place, spot = lax.axis_index("dp"), lax.axis_index("tensor")
    others = []
    for i in range(dp):
        for j in range(tensor):
            if i or j:
                others.append(((place + i) % dp, (spot + j) % tensor))
    greet([{"dp": a, "tensor": b} for a, b in others])
    here = place * tensor + spot
    copies = []
    for n, (a, b) in enumerate(others):
        copies.append(push(parts.at[a], got.at[here], sends, recvs, n, {"dp": a, "tensor": b}))
    got[here] = parts[place]
    for copy in copies:
        copy.wait_recv()
    total[...] = functools.reduce(jnp.add, [got[n] for n in range(dp * tensor)])
    for copy in copies:
        copy.wait_send()


def sum_vectors(parts, ident):
    dp, tensor = lax.axis_size("dp"), lax.axis_size("tensor")
    return pl.pallas_call(
        vectors_kernel,
        in_specs=[vmem()],
        out_specs=vmem(),
        out_shape=jax.ShapeDtypeStruct(parts.shape[1:], jnp.float32),
        scratch_shapes=[
            pltpu.VMEM((dp * tensor,) + parts.shape[1:], jnp.float32),
            pltpu.SemaphoreType.DMA((dp * tensor - 1,)), pltpu.SemaphoreType.DMA((dp * tensor - 1,)),
        ],
        compiler_params=remote_params(ident),
        name="sum_vectors",
    )(parts)


def normalize(values):
    mean = jnp.mean(values, axis=-1, keepdims=True)
    centred = values - mean
    spread = jnp.mean(centred * centred, axis=-1, keepdims=True)
    factor = lax.rsqrt(spread + 1e-05)
    return (centred * factor, factor)


def norm_back(grad_out, normed, factor, gain):
    scaled = grad_out * gain
    first = jnp.mean(scaled, axis=-1, keepdims=True)
    second = jnp.mean(scaled * normed, axis=-1, keepdims=True)
    return factor * (scaled - first - normed * second)


def gelu_tanh(values):
    return jax.nn.gelu(values, approximate=True)


def inner_rows(left, right):
    return lax.dot_general(
        left, right, (((0,), (0,)), ((), ())), preferred_element_type=jnp.float32
    )


def scatter_dp(grad):
    return lax.psum_scatter(grad.astype(jnp.bfloat16), "dp", scatter_dimension=0, tiled=True).astype(jnp.float32)


def spread(vectors, dp):
    depth = vectors.shape[1]
    owner = jnp.arange(dp * depth, dtype=jnp.int32) // depth
    return jnp.where(owner[None, :] == lax.axis_index("dp"), jnp.tile(vectors, (1, dp)), 0.0)


def on_device(
    tokens, cotangent, lengths, w_qkv, w_out, w_fc, w_proj, ln1_gain, ln1_bias, ln2_gain, ln2_bias
):
    dp = lax.axis_size("dp")
    low = jnp.bfloat16
    depth, _, local = w_qkv.shape
    width = depth * dp
    heads = local // HEAD
    small_dp = dp <= 8 and depth % 16 == 0
    columns = 3 * local
    inputs = tokens.astype(jnp.float32)
    vectors = jnp.stack([ln1_gain, ln1_bias, ln2_gain, ln2_bias]).astype(jnp.float32)
    shard = jnp.concatenate([w_qkv.reshape(depth, columns), w_out.T], axis=1)
    if small_dp:
        placed = jnp.concatenate([spread(vectors, dp), jnp.zeros((4, width), jnp.float32)])
        all_norm1, projected, weights, gains = opening(tokens, placed, shard, columns, 0)
    else:
        gains = lax.psum(spread(vectors, dp), "dp")
        weights = lax.all_gather(shard, "dp", axis=0, tiled=True)
        lowered1 = (normalize(inputs)[0] * gains[0] + gains[1]).astype(low)
        all_norm1, projected = gather_times(lowered1, weights[:, :columns], low, 0)
    out_turned = weights[:, columns:]
    w_fc, lengths, projected = lax.optimization_barrier((w_fc, lengths, projected))
    fc_full = lax.all_gather(w_fc, "dp", axis=0, tiled=True)
    cotangent_late, fc_full = lax.optimization_barrier((cotangent, fc_full))
    grad_all = lax.all_gather(cotangent_late, "tensor", axis=0, tiled=True)
    gain1, gain2, bias2 = gains[0], gains[2], gains[3]
    mixed, sums = attend(projected, lengths, heads)
    if small_dp:
        attended, proj_turned = scatter_times(mixed, out_turned, 1, shard=w_proj.T)
    else:
        attended = scatter_times(mixed, out_turned, 1)[0]
        proj_turned = lax.all_gather(w_proj.T, "dp", axis=0, tiled=True)
    resid = inputs + attended
    normed2, factor2 = normalize(resid)
    lowered2 = (normed2 * gain2 + bias2).astype(low)
    all_norm2, hidden_pre = gather_times(lowered2, fc_full, jnp.float32, 2)
    hidden, gelu_pull = jax.vjp(gelu_tanh, hidden_pre)
    hidden_low = hidden.astype(low)
    hidden_grad = nn(grad_all, proj_turned)
    proj_grad = inner_rows(grad_all, hidden_low).astype(low)
    pre_low = gelu_pull(hidden_grad)[0].astype(low)
    fc_grad = inner_rows(all_norm2, pre_low).astype(low)
    if small_dp:
        norm2_grad, proj_sum = scatter_times(pre_low, fc_full, 3, grad=proj_grad)
    else:
        norm2_grad = scatter_times(pre_low, fc_full, 3)[0]
        proj_sum, fc_sum = scatter_dp(proj_grad), scatter_dp(fc_grad)
    gain2_part = jnp.sum(norm2_grad * normed2, axis=0)
    bias2_part = jnp.sum(norm2_grad, axis=0)
    resid_grad = cotangent.astype(jnp.float32) + norm_back(norm2_grad, normed2, factor2, gain2)
    if small_dp:
        resid_all, mixed_grad, fc_sum = gather_times(resid_grad.astype(low), out_turned, low, 4, grad=fc_grad)
    else:
        resid_all, mixed_grad = gather_times(resid_grad.astype(low), out_turned, low, 4)
    hidden_late, mixed_grad = lax.optimization_barrier((hidden_low, mixed_grad))
    mlp_rows = lax.psum_scatter(
        nt(hidden_late, proj_turned).astype(low), "tensor", scatter_dimension=0, tiled=True
    ).astype(jnp.float32)
    block_out = (resid + mlp_rows).astype(low)
    qkv_grad_low = attend_back(projected, mixed, mixed_grad, sums, lengths, heads)
    last_grad = jnp.concatenate(
        [inner_rows(all_norm1, qkv_grad_low).astype(low), inner_rows(resid_all, mixed).astype(low)], axis=1
    )
    if small_dp:
        norm1_grad, last_sum = scatter_times(qkv_grad_low, weights[:, :columns], 5, grad=last_grad)
    else:
        norm1_grad = scatter_times(qkv_grad_low, weights[:, :columns], 5)[0]
        last_sum = scatter_dp(last_grad)
    normed1, factor1 = normalize(inputs)
    input_grad = (resid_grad + norm_back(norm1_grad, normed1, factor1, gain1)).astype(low)
    parts = jnp.stack([jnp.sum(norm1_grad * normed1, axis=0), jnp.sum(norm1_grad, axis=0), gain2_part, bias2_part])
    if small_dp:
        pieces = jnp.pad(parts.reshape(4, dp, depth).transpose(1, 0, 2), ((0, 0), (0, 4), (0, -depth % 128)))
        shares = sum_vectors(pieces, 6)[:4, :depth]
    else:
        shares = lax.psum(lax.psum_scatter(parts, "dp", scatter_dimension=1, tiled=True), "tensor")
    return (
        block_out,
        input_grad,
        last_sum[:, :columns].reshape(depth, 3, local),
        last_sum[:, columns:].T,
        fc_sum,
        proj_sum.T,
        shares[0],
        shares[1],
        shares[2],
        shares[3],
    )


def solution(mesh):
    placed = (
        P(("dp", "tensor"), None),
        P(("dp", "tensor"), None),
        P("dp", None),
        P("dp", None, "tensor"),
        P("tensor", "dp"),
        P("dp", "tensor"),
        P("tensor", "dp"),
        P("dp"),
        P("dp"),
        P("dp"),
        P("dp"),
    )
    return jax.shard_map(
        on_device,
        mesh=mesh,
        in_specs=placed,
        out_specs=(
            P(("dp", "tensor"), None),
            P(("dp", "tensor"), None),
            P("dp", None, "tensor"),
            P("tensor", "dp"),
            P("dp", "tensor"),
            P("tensor", "dp"),
            P("dp"),
            P("dp"),
            P("dp"),
            P("dp"),
        ),
        check_vma=False,
    )
```
